256 devices in a mesh: leaf: 16 (over y, x), blk: 16 (over z, core).
Axes of the slice: x: 4, y: 4, z: 8, core: 2. Of those that a mesh axis runs over, the one named last changes fastest.
Arguments:
- leaf_rhs: bfloat16 [81920, 256], P(('leaf', 'blk')), may hold values from -6 to 6
- leaf_inverse: bfloat16 [81920, 5120], P(('leaf', 'blk')), may hold values from -0.078125 to 0.078125
- leaf_lower: bfloat16 [32768, 5120], P(('leaf', 'blk')), may hold values from -0.078125 to 0.078125
- sep_rhs: bfloat16 [4, 16384, 256], P(None, ('leaf', 'blk')), may hold values from -6 to 6
- sep_inverse: bfloat16 [16384, 30720], P(('leaf', 'blk'))
- sep_lower: bfloat16 [32768, 14336], P(('leaf', 'blk'))
- slot_map: int32 [4, 256, 2], P(None, ('leaf', 'blk')), may hold values from 0 to 5, as said below
Outputs:
- leaf_solution: bfloat16 [81920, 256], P(('leaf', 'blk'))
- sep_solution: bfloat16 [4, 16384, 256], P(None, ('leaf', 'blk'))
The draws below stay inside these ranges and needn't reach their ends.
Inputs may be any that keep to these rules, and one draw needn't show every extreme that they name: For every level below the top, slot_map[h-1, q] holds two different numbers of 0 to 5; at the top level it holds 0 and 1 in some order.
All inputs are finite; a program needn't handle non-finite values.
Results may differ from the reference program's by a relative error of at most 0.015.
Values may be sent and summed in bfloat16 or wider, within the bound.
A program may use at most 128 MiB of HBM per device.

```python
import jax
import jax.numpy as jnp
from jax import lax

RHS = 256
PIV_DEV = 64
UPD_DEV = 128
LV = 4
POS = 256
SN0 = 5120
SEP_UNIT = 1024
SEP_COLS = 30720
LOW_COLS = 14336
LEAF_ROWS = 81920
LOW_ROWS = 32768
SEP_ROWS = 16384
N_LEAF = 16
N_BLK = 16


def column_scale(columns_total):
    col_index = jnp.arange(columns_total, dtype=jnp.int32)
    height = jnp.zeros((columns_total,), jnp.float32)
    for step_index in range(1, LV + 1):
        height = height + (col_index >= SEP_UNIT * (2 ** step_index - 2)).astype(jnp.float32)
    return jax.lax.rsqrt(SEP_UNIT * jnp.exp2(height))


def scaled_block(key, row_count, columns_total):
    values = jax.random.normal(key, (row_count, columns_total), jnp.float32)
    return (values * column_scale(columns_total)[None, :]).astype(jnp.bfloat16)


def draw_sep_inverse(key, part):
    return scaled_block(jax.random.fold_in(key, 11), POS * PIV_DEV, SEP_COLS)


def draw_sep_lower(key, part):
    return scaled_block(jax.random.fold_in(key, 13), POS * UPD_DEV, LOW_COLS)


def draw_slot_map(key, part):
    scores = jax.random.randint(jax.random.fold_in(key, 17), (LV, POS, 6), 0, 1 << 26) * 8 + jnp.arange(6, dtype=jnp.int32)
    heights = jnp.arange(LV, dtype=jnp.int32)[:, None, None]
    blocked = (heights == LV - 1) & (jnp.arange(6, dtype=jnp.int32)[None, None, :] >= 2)
    scores = jnp.where(blocked, 1 << 30, scores)
    ordering = jnp.argsort(scores, axis=-1)
    return ordering[:, :, :2].astype(jnp.int32)


def steps_of(stream_key, dims, cuts, least, top_value):
    level = 1.0
    for dim, shards_of in cuts:
        steps = jax.random.uniform(jax.random.fold_in(jax.random.fold_in(stream_key, 6), dim), (shards_of,), jnp.float32, least / len(cuts), top_value / len(cuts))
        level = level * jnp.repeat(jnp.exp(steps), dims[dim] // shards_of).reshape((-1,) + (1,) * (len(dims) - 1 - dim))
    return level


def bell_draw(stream_key, extent, spread, most, split=(), kind=jnp.bfloat16):
    level = steps_of(stream_key, extent, split, -0.22, 0.18) if split else 1.0
    array = jax.random.normal(stream_key, extent, jnp.float32) * spread * level
    return jnp.minimum(jnp.maximum(array, -most), most).astype(kind)


def setup_inputs(seed: int = 0) -> dict:
    streams_of = jax.random.split(jax.random.key(seed), 8)
    leaf_rhs = bell_draw(streams_of[0], (LEAF_ROWS, RHS), 1.0, 6.0, ((0, 256),))
    leaf_inverse = bell_draw(streams_of[1], (LEAF_ROWS, SN0), SN0 ** -0.5, 0.078125, ((0, 256),))
    leaf_lower = bell_draw(streams_of[2], (LOW_ROWS, SN0), SN0 ** -0.5, 0.078125, ((0, 256),))
    sep_rhs = bell_draw(streams_of[3], (LV, SEP_ROWS, RHS), 1.0, 6.0, ((1, 256),))
    sep_inverse = draw_sep_inverse(jax.random.fold_in(streams_of[7], 71), 0)
    sep_lower = draw_sep_lower(jax.random.fold_in(streams_of[7], 71), 0)
    slot_map = draw_slot_map(jax.random.fold_in(streams_of[7], 71), 0)
    return dict(leaf_rhs=leaf_rhs, leaf_inverse=leaf_inverse, leaf_lower=leaf_lower, sep_rhs=sep_rhs, sep_inverse=sep_inverse, sep_lower=sep_lower, slot_map=slot_map)


HIGH = lax.Precision.HIGHEST


def product_f32(matrix, vectors):
    return jnp.dot(matrix.astype(jnp.float32), vectors.astype(jnp.float32), precision=HIGH)


def leaf_node(operands):
    inverse, lower_part, front_rows = operands
    solved = product_f32(inverse, front_rows).astype(jnp.bfloat16)
    return solved, -product_f32(lower_part, solved)


def node_solve(operands):
    return product_f32(operands[0], operands[1]).astype(jnp.bfloat16)


def node_reduce(operands):
    return product_f32(operands[0], operands[1])


def reference(leaf_rhs, leaf_inverse, leaf_lower, sep_rhs, sep_inverse, sep_lower, slot_map):
    leaf_front = leaf_rhs.reshape(N_LEAF, SN0, RHS)
    leaf_inv = leaf_inverse.reshape(N_LEAF, SN0, SN0)
    leaf_low = leaf_lower.reshape(N_LEAF, UPD_DEV * N_BLK, SN0)
    leaf_solution, update = lax.map(leaf_node, (leaf_inv, leaf_low, leaf_front))
    update = update.reshape(POS, 2, PIV_DEV, RHS)
    solutions = []
    for height in range(1, LV + 1):
        at_root = height == LV
        front_slots = 1 if at_root else 3
        targets = slot_map[height - 1]
        onehot = (targets[:, :, None] == jnp.arange(2 * front_slots, dtype=jnp.int32)[None, None, :]).astype(jnp.float32)
        mixed = jnp.einsum("qst,qspr->qtpr", onehot, update, precision=HIGH)
        own_part = mixed[:, :front_slots]
        sent_part = mixed[:, front_slots:]
        partner = jnp.bitwise_xor(jnp.arange(POS, dtype=jnp.int32), N_BLK * 2 ** (height - 1))
        front_rows = own_part + sent_part[partner]
        pivots = (sep_rhs[height - 1].reshape(POS, PIV_DEV, RHS).astype(jnp.float32) + front_rows[:, 0]).astype(jnp.bfloat16)
        width_now = SEP_UNIT * 2 ** height
        offset = SEP_UNIT * (2 ** height - 2)
        node_count = (POS * PIV_DEV) // width_now
        inverse = sep_inverse[:, offset:offset + width_now].reshape(node_count, width_now, width_now)
        solved = lax.map(node_solve, (inverse, pivots.reshape(node_count, width_now, RHS)))
        solutions.append(solved.reshape(POS * PIV_DEV, RHS))
        if not at_root:
            lower_part = sep_lower[:, offset:offset + width_now].reshape(node_count, 2 * width_now, width_now)
            product = lax.map(node_reduce, (lower_part, solved))
            remaining = front_rows[:, 1:].reshape(node_count, 2 * width_now, RHS)
            update = (remaining - product).reshape(POS, 2, PIV_DEV, RHS)
    return leaf_solution.reshape(N_LEAF * SN0, RHS), jnp.stack(solutions)
```

```python
import functools

import jax
import jax.numpy as jnp
from jax import lax
from jax.experimental import pallas as pl
from jax.experimental.pallas import tpu as pltpu
from jax.sharding import PartitionSpec as P

MESH = pl.DeviceIdType.MESH
F32 = jnp.float32
BF16 = jnp.bfloat16
CORES = 2
CHUNK = 64


def flipped(index, mask):
    result = index
    bit = 1
    while bit <= mask:
        if mask & bit:
            result = result + (bit - 2 * bit * lax.rem(lax.div(index, bit), 2))
        bit *= 2
    return result


def take(ref, sem):
    pltpu.make_async_copy(ref, ref, sem).wait()


def rows(start, count):
    return pl.ds(pl.multiple_of(start, count), count)


def kernel(
    sizes,
    leaf_rhs,
    leaf_inverse,
    leaf_lower,
    sep_rhs,
    sep_inverse,
    sep_lower,
    slot_map,
    leaf_out,
    sep_out,
    inv_v,
    low_v,
    rhs_v,
    a_v,
    l_v,
    x_leaf,
    acc,
    x_sep,
    part_own,
    part_send,
    part_recv,
    update,
    swap_send,
    swap_recv,
    kept,
    load_sem,
    out_sem,
    ring_sem,
    leaf_sib_sem,
    leaf_send_sem,
    z_sem,
    sib_sem,
    gather_send_sem,
    part_recv_sem,
    part_send_sem,
    swap_recv_sem,
    swap_send_sem,
    bulk_recv_sem,
    bulk_send_sem,
):
    n_leaf, n_blk, levels = sizes
    nz = n_blk // CORES
    half = nz // 2
    leaf = lax.axis_index("leaf")
    blk = lax.axis_index("blk")
    z = lax.div(blk, CORES)
    core = lax.rem(blk, CORES)
    sibling = (leaf, flipped(blk, 1))
    leaf_rows, columns = leaf_rhs.shape
    chunks = leaf_rows // CHUNK
    piv = sep_rhs.shape[1]
    base = piv * n_blk

    def at_z(distance):
        return lax.rem(z + (distance + nz), nz)

    loads = [
        pltpu.make_async_copy(
            leaf_rhs, x_leaf[0].at[rows(blk * leaf_rows, leaf_rows)], load_sem.at[0]
        ),
        pltpu.make_async_copy(leaf_inverse, inv_v, load_sem.at[1]),
        pltpu.make_async_copy(leaf_lower, low_v, load_sem.at[2]),
        pltpu.make_async_copy(sep_rhs, rhs_v, load_sem.at[3]),
    ]
    own_a, own_l = [], []
    for h in range(1, levels + 1):
        offset = base * (2**h - 2) + base * lax.rem(leaf, 2**h)
        cols = pl.ds(pl.multiple_of(offset, base), base)
        own_a.append(
            pltpu.make_async_copy(
                sep_inverse.at[:, cols], a_v[h - 1].at[pl.ds(0, piv)], load_sem.at[2 + 2 * h]
            )
        )
        if h < levels:
            own_l.append(
                pltpu.make_async_copy(
                    sep_lower.at[:, cols],
                    l_v[h - 1].at[pl.ds(0, 2 * piv)],
                    load_sem.at[3 + 2 * h],
                )
            )
    for copy in loads + own_a + own_l:
        copy.start()

    barrier = pltpu.get_barrier_semaphore()
    peers = [sibling]
    peers += [(leaf, at_z(d) * CORES + core) for d in range(1, nz)]
    peers += [(flipped(leaf, m), blk) for m in range(1, n_leaf)]
    for peer in peers:
        pl.semaphore_signal(barrier, inc=1, device_id=peer, device_id_type=MESH)
    pl.semaphore_wait(barrier, len(peers))

    def send(src, dst, send_sem, recv_sem, device):
        pltpu.make_async_remote_copy(
            src_ref=src,
            dst_ref=dst,
            send_sem=send_sem,
            recv_sem=recv_sem,
            device_id=device,
            device_id_type=MESH,
        ).start()

    def send_blocks(kind, h, masks):
        source = sep_inverse if kind == 0 else sep_lower
        target = a_v[h - 1] if kind == 0 else l_v[h - 1]
        count = piv if kind == 0 else 2 * piv
        index = 2 * (h - 1) + kind
        for m in masks:
            peer = flipped(leaf, m)
            offset = base * (2**h - 2) + base * lax.rem(peer, 2**h)
            send(
                source.at[:, pl.ds(pl.multiple_of(offset, base), base)],
                target.at[pl.ds(m * count, count)],
                bulk_send_sem.at[index],
                bulk_recv_sem.at[index],
                (peer, blk),
            )

    def wait_blocks(kind, h):
        target = a_v[h - 1] if kind == 0 else l_v[h - 1]
        count = piv if kind == 0 else 2 * piv
        (own_a if kind == 0 else own_l)[h - 1].wait()
        take(
            target.at[pl.ds(count, count * (2**h - 1))],
            bulk_recv_sem.at[2 * (h - 1) + kind],
        )

    def leaf_gather(phase, multiply, after_start):
        x = x_leaf[phase]
        send_sem = leaf_send_sem.at[phase]

        def chunk_at(slot, chunk):
            return x.at[rows((slot * CORES + core) * leaf_rows + chunk * CHUNK, CHUNK)]

        def hop(way, step, chunk):
            sign = 1 if way == 0 else -1
            block = chunk_at(at_z(-sign * (step - 1)), chunk)
            send(
                block,
                block,
                send_sem,
                ring_sem.at[phase, way, step - 1, chunk],
                (leaf, at_z(sign) * CORES + core),
            )

        def to_sibling(slot, sem_index, chunk):
            block = chunk_at(slot, chunk)
            send(block, block, send_sem, leaf_sib_sem.at[phase, sem_index], sibling)

        def arrived(way, step, chunk):
            sign = 1 if way == 0 else -1
            slot = at_z(-sign * step)
            take(chunk_at(slot, chunk), ring_sem.at[phase, way, step - 1, chunk])
            to_sibling(slot, (nz - step) if way == 0 else step, chunk)

        def each(first, last, body):
            def run(chunk, carry):
                body(chunk)
                return carry

            lax.fori_loop(first, last, run, 0)

        split = (chunks + 1) // 2

        def begin(chunk):
            hop(0, 1, chunk)
            hop(1, 1, chunk)
            to_sibling(z, 0, chunk)

        each(0, chunks, begin)
        after_start()

        def finish(distance):
            take(x.at[rows(0, leaf_rows)], leaf_sib_sem.at[phase, distance % nz])
            multiply(at_z(distance))

        finish(0)
        for step in range(1, half):
            if step + 1 < half:

                def both(chunk, step=step):
                    for way in (0, 1):
                        arrived(way, step, chunk)
                        hop(way, step + 1, chunk)

                each(0, chunks, both)
            else:

                def low(chunk, step=step):
                    arrived(0, step, chunk)
                    hop(0, step + 1, chunk)
                    arrived(1, step, chunk)

                def high(chunk, step=step):
                    arrived(1, step, chunk)
                    hop(1, step + 1, chunk)
                    arrived(0, step, chunk)

                each(0, split, low)
                each(split, chunks, high)
            finish(-step)
            finish(step)
        each(0, split, lambda chunk: arrived(0, half, chunk))
        each(split, chunks, lambda chunk: arrived(1, half, chunk))
        finish(half)

    def leaf_gather_sent(phase):
        total = chunks * (2 * nz - 1) * CHUNK
        take(x_leaf[phase].at[pl.ds(0, total)], leaf_send_sem.at[phase])

    chip_rows = leaf_rows * CORES

    loads[0].wait()

    def multiply_inverse(slot):
        span = rows(slot * chip_rows, chip_rows)
        acc[...] += jnp.dot(
            inv_v[:, span], x_leaf[0][span, :], preferred_element_type=F32
        )

    def multiply_lower(slot):
        span = rows(slot * chip_rows, chip_rows)
        update[...] -= jnp.dot(
            low_v[:, span], x_leaf[1][span, :], preferred_element_type=F32
        )

    def first_bulk():
        for h in (1, 2):
            if h <= levels:
                send_blocks(0, h, range(1, 2**h))
                if h < levels:
                    send_blocks(1, h, range(1, 2**h))
        acc[...] = jnp.zeros_like(acc)
        loads[1].wait()

    def second_bulk():
        if levels >= 3:
            send_blocks(0, 3, range(1, 8))
        update[...] = jnp.zeros_like(update)
        loads[2].wait()

    leaf_gather(0, multiply_inverse, first_bulk)
    own_leaf = rows(blk * leaf_rows, leaf_rows)
    x_leaf[1][own_leaf, :] = acc[...].astype(BF16)
    leaf_gather(1, multiply_lower, second_bulk)
    out_copies = [
        pltpu.make_async_copy(x_leaf[1].at[own_leaf], leaf_out, out_sem.at[0])
    ]
    out_copies[0].start()

    def gather(g, after_start):
        x = x_sep[g]

        def block(slot):
            return x.at[rows((slot * CORES + core) * piv, piv)]

        near = sorted(range(1, nz), key=lambda d: min(d, nz - d))
        for d in reversed(near):
            send(
                block(z),
                block(z),
                gather_send_sem.at[g],
                z_sem.at[g, d],
                (leaf, at_z(d) * CORES + core),
            )
        send(block(z), block(z), gather_send_sem.at[g], sib_sem.at[g], sibling)
        after_start()
        for d in near:
            slot = at_z(-d)
            take(block(slot), z_sem.at[g, d])
            send(block(slot), block(slot), gather_send_sem.at[g], sib_sem.at[g], sibling)
        take(x.at[pl.ds(0, nz * piv)], sib_sem.at[g])

    def gather_sent(g):
        take(x_sep[g].at[pl.ds(0, (2 * nz - 1) * piv)], gather_send_sem.at[g])

    def products(g, matrix, count, h):
        members = 2**h
        per = max(1, min(members, 256 // count))
        out, own = part_send[g], part_own.at[pl.ds(0, count)]
        x = x_sep[g]
        for first in reversed(range(0, members, per)):
            span = pl.ds(first * count, per * count)
            value = jnp.dot(matrix[span, :], x[...], preferred_element_type=F32)
            out[span, :] = value.astype(BF16)
            if first == 0:
                own[...] = value[:count]
            for m in range(max(first, 1), first + per):
                slot = pl.ds(m * count, count)
                send(
                    out.at[slot],
                    part_recv[g].at[slot],
                    part_send_sem.at[g],
                    part_recv_sem.at[g],
                    (flipped(leaf, m), blk),
                )
        take(part_recv[g].at[pl.ds(count, (members - 1) * count)], part_recv_sem.at[g])
        total = own[...]
        for m in range(1, members):
            total += part_recv[g][pl.ds(m * count, count), :].astype(F32)
        return total

    def products_sent(g, count, h):
        take(part_send[g].at[pl.ds(count, (2**h - 1) * count)], part_send_sem.at[g])

    later = {}
    if levels >= 4:
        later = {
            0: lambda: send_blocks(1, 3, range(1, 4)),
            1: lambda: send_blocks(1, 3, range(4, 8)),
            2: lambda: send_blocks(0, 4, range(1, 6)),
            3: lambda: send_blocks(0, 4, range(6, 11)),
            4: lambda: send_blocks(0, 4, range(11, 16)),
        }

    loads[3].wait()
    own_row = rows(blk * piv, piv)
    for h in range(1, levels + 1):
        at_root = h == levels
        slots = 1 if at_root else 3
        g = 2 * (h - 1)
        partner = (flipped(leaf, 2 ** (h - 1)), blk)

        def mixed(t):
            total = None
            for s in (0, 1):
                weight = jnp.where(slot_map[h - 1, 0, s] == t, 1.0, 0.0).astype(F32)
                term = update[pl.ds(s * piv, piv), :] * weight
                total = term if total is None else total + term
            return total

        def swap(index, start, count):
            span = pl.ds(start, count)
            send(
                swap_send[h - 1].at[span],
                swap_recv[h - 1].at[span],
                swap_send_sem.at[h - 1, index],
                swap_recv_sem.at[h - 1, index],
                partner,
            )

        swap_send[h - 1][pl.ds(0, piv), :] = mixed(slots).astype(BF16)
        swap(0, 0, piv)
        if not at_root:
            for t in (1, 2):
                swap_send[h - 1][pl.ds(t * piv, piv), :] = mixed(slots + t).astype(BF16)
            swap(1, piv, 2 * piv)
            for t in (1, 2):
                kept[pl.ds((t - 1) * piv, piv), :] = mixed(t)
        own_front = mixed(0)
        take(swap_recv[h - 1].at[pl.ds(0, piv)], swap_recv_sem.at[h - 1, 0])
        front = own_front + swap_recv[h - 1][pl.ds(0, piv), :].astype(F32)
        x_sep[g][own_row, :] = (rhs_v[h - 1].astype(F32) + front).astype(BF16)
        gather(g, later.get(g, lambda: None))
        wait_blocks(0, h)
        solved = products(g, a_v[h - 1], piv, h).astype(BF16)
        last = g + 1
        x_sep[last][own_row, :] = solved
        out_copies.append(
            pltpu.make_async_copy(
                x_sep[last].at[own_row], sep_out.at[h - 1], out_sem.at[h]
            )
        )
        out_copies[-1].start()
        if not at_root:
            gather(last, later.get(last, lambda: None))
            wait_blocks(1, h)
            product = products(last, l_v[h - 1], 2 * piv, h)
            take(swap_recv[h - 1].at[pl.ds(piv, 2 * piv)], swap_recv_sem.at[h - 1, 1])
            update[...] = (
                kept[...] + swap_recv[h - 1][pl.ds(piv, 2 * piv), :].astype(F32)
            ) - product

    for phase in (0, 1):
        leaf_gather_sent(phase)
    for h in range(1, levels + 1):
        g = 2 * (h - 1)
        gather_sent(g)
        products_sent(g, piv, h)
        take(a_v[h - 1].at[pl.ds(piv, piv * (2**h - 1))], bulk_send_sem.at[g])
        take(swap_send[h - 1].at[pl.ds(0, piv)], swap_send_sem.at[h - 1, 0])
        if h < levels:
            gather_sent(g + 1)
            products_sent(g + 1, 2 * piv, h)
            take(l_v[h - 1].at[pl.ds(2 * piv, 2 * piv * (2**h - 1))], bulk_send_sem.at[g + 1])
            take(swap_send[h - 1].at[pl.ds(piv, 2 * piv)], swap_send_sem.at[h - 1, 1])
    for copy in out_copies:
        copy.wait()


def on_device(sizes, leaf_rhs, leaf_inverse, leaf_lower, sep_rhs, sep_inverse, sep_lower, slot_map):
    n_leaf, n_blk, levels = sizes
    leaf_rows, columns = leaf_rhs.shape
    chunks = leaf_rows // CHUNK
    nz = n_blk // CORES
    piv = sep_rhs.shape[1]
    base = piv * n_blk
    gathers = 2 * levels - 1

    def level_of(g):
        return g // 2 + 1

    def count_of(g):
        return piv * (1 + g % 2)

    vmem, dma = pltpu.VMEM, pltpu.SemaphoreType.DMA
    parts = [vmem((count_of(g) * 2 ** level_of(g), columns), BF16) for g in range(gathers)]
    any_space = pl.BlockSpec(memory_space=pl.ANY)
    return pl.pallas_call(
        functools.partial(kernel, sizes),
        out_shape=(
            jax.ShapeDtypeStruct((leaf_rows, columns), BF16),
            jax.ShapeDtypeStruct((levels, piv, columns), BF16),
        ),
        in_specs=[any_space] * 6 + [pl.BlockSpec(memory_space=pltpu.SMEM)],
        out_specs=(any_space, any_space),
        scratch_shapes=[
            vmem(leaf_inverse.shape, BF16),
            vmem(leaf_lower.shape, BF16),
            vmem(sep_rhs.shape, BF16),
            [vmem((piv * 2**h, base), BF16) for h in range(1, levels + 1)],
            [vmem((2 * piv * 2**h, base), BF16) for h in range(1, levels)],
            [vmem((leaf_rows * n_blk, columns), BF16) for _ in range(2)],
            vmem((leaf_rows, columns), F32),
            [vmem((base, columns), BF16) for _ in range(gathers + 1)],
            vmem((2 * piv, columns), F32),
            parts,
            parts,
            vmem((2 * piv, columns), F32),
            [vmem((3 * piv, columns), BF16) for _ in range(levels)],
            [vmem((3 * piv, columns), BF16) for _ in range(levels)],
            vmem((2 * piv, columns), F32),
            dma((3 + 2 * levels,)),
            dma((1 + levels,)),
            dma((2, 2, nz // 2, chunks)),
            dma((2, nz)),
            dma((2,)),
            dma((gathers, nz)),
            dma((gathers,)),
            dma((gathers,)),
            dma((gathers,)),
            dma((gathers,)),
            dma((levels, 2)),
            dma((levels, 2)),
            dma((gathers,)),
            dma((gathers,)),
        ],
        compiler_params=pltpu.CompilerParams(
            collective_id=0, has_side_effects=True, vmem_limit_bytes=60 * 2**20
        ),
    )(leaf_rhs, leaf_inverse, leaf_lower, sep_rhs, sep_inverse, sep_lower, slot_map)


def solution(mesh):
    n_leaf, n_blk = mesh.shape["leaf"], mesh.shape["blk"]
    sizes = (n_leaf, n_blk, n_leaf.bit_length() - 1)
    return jax.shard_map(
        functools.partial(on_device, sizes),
        mesh=mesh,
        in_specs=(
            P(("leaf", "blk"), None),
            P(("leaf", "blk"), None),
            P(("leaf", "blk"), None),
            P(None, ("leaf", "blk"), None),
            P(("leaf", "blk"), None),
            P(("leaf", "blk"), None),
            P(None, ("leaf", "blk"), None),
        ),
        out_specs=(P(("leaf", "blk"), None), P(None, ("leaf", "blk"), None)),
        check_vma=False,
    )
```

```python
import functools

import jax
import jax.numpy as jnp
from jax import lax
from jax.experimental import pallas as pl
from jax.experimental.pallas import tpu as pltpu
from jax.sharding import PartitionSpec as P

MESH = pl.DeviceIdType.MESH
F32 = jnp.float32
BF16 = jnp.bfloat16
CORES = 2
NX = 4
CHUNK = 64
CHAINS = 2
LEAD = 0.0
LEAF_HOP = 2.9
SIBLING = 0.0
LEAF_SIBLING = 0.0
GATHER = 5.5
SWAP = 2.6
PARTS_A = (2.6, 3.3, 4.5, 6.0)
PARTS_L = (3.0, 4.0, 6.0)
BULK_A3 = 6.0
GATHER_X = (0.5, 0.0)
BULK_ROOM = (8, 8, 8, 8, 0, 0, 0)


def flipped(index, mask):
    result = index
    bit = 1
    while bit <= mask:
        if mask & bit:
            result = result + (bit - 2 * bit * lax.rem(lax.div(index, bit), 2))
        bit *= 2
    return result


def wide_level(h, levels):
    return h == levels


def masks_of(h, levels):
    return [m for m in range(2**h) if not wide_level(h, levels) or m % NX == 0]


def take(ref, sem):
    pltpu.make_async_copy(ref, ref, sem).wait()


def rows(start, count):
    return pl.ds(pl.multiple_of(start, count), count)


def kernel(
    sizes,
    leaf_rhs,
    leaf_inverse,
    leaf_lower,
    sep_rhs,
    sep_inverse,
    sep_lower,
    slot_map,
    leaf_out,
    sep_out,
    inv_v,
    low_v,
    rhs_v,
    map_s,
    a_v,
    l_v,
    chains,
    load_sem,
    bulk_recv_sem,
    bulk_send_sem,
):
    n_leaf, n_blk, levels = sizes
    nz = n_blk // CORES
    half = nz // 2
    leaf = lax.axis_index("leaf")
    blk = lax.axis_index("blk")
    z = lax.div(blk, CORES)
    core = lax.rem(blk, CORES)
    sibling = (leaf, flipped(blk, 1))
    leaf_rows, columns = leaf_rhs.shape
    width = columns // CHAINS
    chunks = leaf_rows // CHUNK
    chip_rows = leaf_rows * CORES
    piv = sep_rhs.shape[1]
    base = piv * n_blk
    own_leaf = rows(blk * leaf_rows, leaf_rows)

    def own_row(h):
        if wide_level(h, levels):
            return rows(lax.rem(leaf, NX) * base + blk * piv, piv)
        return rows(blk * piv, piv)

    def columns_for(h, member):
        index = lax.rem(member, 2**h)
        span = base
        if wide_level(h, levels):
            index, span = lax.div(index, NX), base * NX
        return pl.ds(pl.multiple_of(base * (2**h - 2) + span * index, base), span)

    def at_z(distance):
        return lax.rem(z + (distance + nz), nz)

    def columns_of(c):
        return pl.ds(c * width, width)

    loads = {}

    def load(key, source, target):
        loads[key] = pltpu.make_async_copy(source, target, load_sem.at[len(loads)])
        loads[key].start()

    waited = set()

    def loaded(key):
        if key not in waited:
            waited.add(key)
            loads[key].wait()
            if key[0] in ("a", "l"):
                while any(item[:2] == key for _, item in bulk):
                    send_block(*bulk.pop(0)[1])
                with jax.named_scope(f"blocks{key[0]}{key[1]}"):
                    wait_blocks(*key)

    for c in range(CHAINS):
        load(("rhs", c), leaf_rhs.at[:, columns_of(c)], chains[c]["x_leaf"][0].at[own_leaf])
    load(("inverse",), leaf_inverse, inv_v)
    load(("lower",), leaf_lower, low_v)
    load(("sep_rhs",), sep_rhs, rhs_v)
    load(("map",), slot_map, map_s)
    for h in range(1, levels + 1):
        own = columns_for(h, leaf)
        load(("a", h), sep_inverse.at[:, own], a_v[h - 1].at[pl.ds(0, piv)])
        if h < levels:
            load(("l", h), sep_lower.at[:, own], l_v[h - 1].at[pl.ds(0, 2 * piv)])

    barrier = pltpu.get_barrier_semaphore()
    peers = [sibling]
    peers += [(leaf, at_z(d) * CORES + core) for d in range(1, nz)]
    peers += [(flipped(leaf, m), blk) for m in range(1, n_leaf)]
    for peer in peers:
        pl.semaphore_signal(barrier, inc=1, device_id=peer, device_id_type=MESH)
    for c in range(CHAINS):
        loaded(("rhs", c))
    with jax.named_scope("entry"):
        pl.semaphore_wait(barrier, len(peers))

    def send(src, dst, send_sem, recv_sem, device):
        pltpu.make_async_remote_copy(
            src_ref=src,
            dst_ref=dst,
            send_sem=send_sem,
            recv_sem=recv_sem,
            device_id=device,
            device_id_type=MESH,
        ).start()

    def matrix_of(kind, h):
        if kind == "a":
            return sep_inverse, a_v[h - 1], piv, 2 * (h - 1)
        return sep_lower, l_v[h - 1], 2 * piv, 2 * (h - 1) + 1

    def send_block(kind, h, m, first, size):
        source, target, count, index = matrix_of(kind, h)
        peer = flipped(leaf, m)
        size = min(size, count)
        slot = masks_of(h, levels).index(m)
        send(
            source.at[pl.ds(first, size), columns_for(h, peer)],
            target.at[pl.ds(slot * count + first, size)],
            bulk_send_sem.at[index],
            bulk_recv_sem.at[index],
            (peer, blk),
        )

    def wait_blocks(kind, h):
        source, target, count, index = matrix_of(kind, h)
        others = len(masks_of(h, levels)) - 1
        take(target.at[pl.ds(count, count * others)], bulk_recv_sem.at[index])

    def blocks_beside(g):
        room = BULK_ROOM[g]
        while bulk and room > 0:
            item = bulk.pop(0)[1]
            send_block(*item)
            room -= (0, 1, 2, 1)[item[2] % 4]

    def each(first, last, body):
        def run(chunk, carry):
            body(chunk)
            return carry

        lax.fori_loop(first, last, run, 0)

    def leaf_gather(c, phase, multiply):
        own = chains[c]
        x = own["x_leaf"][phase]
        send_sem = own["leaf_send_sem"].at[phase]

        def chunk_at(slot, chunk):
            return x.at[rows((slot * CORES + core) * leaf_rows + chunk * CHUNK, CHUNK)]

        def hop(way, step, chunk):
            sign = 1 if way == 0 else -1
            block = chunk_at(at_z(-sign * (step - 1)), chunk)
            send(
                block,
                block,
                send_sem,
                own["ring_sem"].at[phase, way, step - 1, chunk],
                (leaf, at_z(sign) * CORES + core),
            )

        def to_sibling(slot, sem_index, chunk):
            block = chunk_at(slot, chunk)
            send(block, block, send_sem, own["leaf_sib_sem"].at[phase, sem_index], sibling)

        def arrived(way, step, chunk):
            sign = 1 if way == 0 else -1
            slot = at_z(-sign * step)
            take(chunk_at(slot, chunk), own["ring_sem"].at[phase, way, step - 1, chunk])
            to_sibling(slot, (nz - step) if way == 0 else step, chunk)

        split = (chunks + c) // 2 if CHAINS > 1 else (chunks + 1) // 2

        def begin(chunk):
            hop(0, 1, chunk)
            hop(1, 1, chunk)
            to_sibling(z, 0, chunk)

        def finish(distance):
            take(x.at[rows(0, leaf_rows)], own["leaf_sib_sem"].at[phase, distance % nz])
            multiply(at_z(distance), distance == 0)

        each(0, chunks, begin)
        yield LEAF_HOP
        for step in range(1, half):
            with jax.named_scope(f"leaf{phase}c{c}s{step}"):
                if step + 1 < half:

                    def both(chunk, step=step):
                        for way in (0, 1):
                            arrived(way, step, chunk)
                            hop(way, step + 1, chunk)

                    each(0, chunks, both)
                else:

                    def low(chunk, step=step):
                        arrived(0, step, chunk)
                        hop(0, step + 1, chunk)
                        arrived(1, step, chunk)

                    def high(chunk, step=step):
                        arrived(1, step, chunk)
                        hop(1, step + 1, chunk)
                        arrived(0, step, chunk)

                    each(0, split, low)
                    each(split, chunks, high)
            with jax.named_scope(f"leafm{phase}c{c}s{step}"):
                if step == 1:
                    finish(0)
                else:
                    finish(1 - step)
                    finish(step - 1)
            yield LEAF_HOP
        with jax.named_scope(f"leaf{phase}c{c}s{half}"):
            each(0, split, lambda chunk: arrived(0, half, chunk))
            each(split, chunks, lambda chunk: arrived(1, half, chunk))
        if half > 1:
            finish(1 - half)
            finish(half - 1)
        else:
            finish(0)
        yield LEAF_SIBLING
        with jax.named_scope(f"leafm{phase}c{c}s{half}"):
            finish(half)

    def gather(c, g, h, name):
        own = chains[c]
        wide = wide_level(h, levels)
        x = own["x_sep"][g]
        part = lax.rem(leaf, NX) * base if wide else 0

        def block(slot, start=part):
            return x.at[rows(start + (slot * CORES + core) * piv, piv)]

        def push(ref, sem, device):
            send(ref, ref, own["gather_send_sem"].at[g], sem, device)

        def to_sibling(ref):
            push(ref, own["sib_sem"].at[g], sibling)

        near = sorted(range(1, nz), key=lambda d: min(d, nz - d))
        halves = ([0] + near[: nz // 2 - 1], near[nz // 2 - 1 :])

        def along_x(d):
            if wide:
                for m in (1, 3, 2):
                    if m < NX:
                        sem = own["x_sem"].at[m, 0 if d in halves[0] else 1]
                        push(block(at_z(-d)), sem, (flipped(leaf, m), blk))

        for d in reversed(near):
            push(block(z), own["z_sem"].at[g, d], (leaf, at_z(d) * CORES + core))
        to_sibling(block(z))
        along_x(0)
        if c == CHAINS - 1:
            blocks_beside(g)

        yield GATHER
        with jax.named_scope(f"far{name}c{c}"):
            for d in near:
                take(block(at_z(-d)), own["z_sem"].at[g, d])
                along_x(d)
                to_sibling(block(at_z(-d)))
        if wide:
            for half_index in (0, 1):
                yield GATHER_X[half_index]
                with jax.named_scope(f"x{half_index}{name}c{c}"):
                    for m in (1, 3, 2):
                        if m < NX:
                            take(
                                x.at[pl.ds(0, len(halves[half_index]) * piv)],
                                own["x_sem"].at[m, half_index],
                            )
                            start = lax.rem(flipped(leaf, m), NX) * base
                            for d in halves[half_index]:
                                to_sibling(block(at_z(-d), start))
        yield SIBLING
        with jax.named_scope(f"sib{name}c{c}"):
            take(x.at[pl.ds(0, nz * piv * (NX if wide else 1))], own["sib_sem"].at[g])

    def products(c, g, matrix, count, h):
        own = chains[c]
        masks = masks_of(h, levels)
        members = len(masks)
        per = max(1, min(members, 256 // count))
        out, mine = own["part_send"][g], own["part_own"].at[pl.ds(0, count)]
        x = own["x_sep"][g]
        for first in reversed(range(0, members, per)):
            span = pl.ds(first * count, per * count)
            value = jnp.dot(matrix[span, :], x[...], preferred_element_type=F32)
            out[span, :] = value.astype(BF16)
            if first == 0:
                mine[...] = value[:count]
            for m in range(max(first, 1), first + per):
                slot = pl.ds(m * count, count)
                send(
                    out.at[slot],
                    own["part_recv"][g].at[slot],
                    own["part_send_sem"].at[g],
                    own["part_recv_sem"].at[g],
                    (flipped(leaf, masks[m]), blk),
                )

    def summed(c, g, count, h, name):
        own = chains[c]
        members = len(masks_of(h, levels))
        with jax.named_scope(f"parts{name}c{c}"):
            take(
                own["part_recv"][g].at[pl.ds(count, (members - 1) * count)],
                own["part_recv_sem"].at[g],
            )
        total = own["part_own"][pl.ds(0, count), :]
        for m in range(1, members):
            total += own["part_recv"][g][pl.ds(m * count, count), :].astype(F32)
        return total

    out_copies = []

    def write(source, target, sem):
        out_copies.append(pltpu.make_async_copy(source, target, sem))
        out_copies[-1].start()

    def chain(c):
        own = chains[c]
        cols = columns_of(c)
        acc, update, kept = own["acc"], own["update"], own["kept"]

        def multiply_inverse(slot, first):
            loaded(("inverse",))
            span = rows(slot * chip_rows, chip_rows)
            value = jnp.dot(inv_v[:, span], own["x_leaf"][0][span, :], preferred_element_type=F32)
            acc[...] = value if first else acc[...] + value

        def multiply_lower(slot, first):
            loaded(("lower",))
            span = rows(slot * chip_rows, chip_rows)
            value = jnp.dot(low_v[:, span], own["x_leaf"][1][span, :], preferred_element_type=F32)
            update[...] = -value if first else update[...] - value

        yield from leaf_gather(c, 0, multiply_inverse)
        own["x_leaf"][1][own_leaf, :] = acc[...].astype(BF16)
        yield from leaf_gather(c, 1, multiply_lower)
        write(own["x_leaf"][1].at[own_leaf], leaf_out.at[:, cols], own["out_sem"].at[0])

        for h in range(1, levels + 1):
            at_root = h == levels
            slots = 1 if at_root else 3
            g = 2 * (h - 1)
            partner = (flipped(leaf, 2 ** (h - 1)), blk)
            swap_send, swap_recv = own["swap_send"][h - 1], own["swap_recv"][h - 1]
            loaded(("map",))
            loaded(("sep_rhs",))

            def mixed(t):
                total = None
                for s in (0, 1):
                    weight = jnp.where(map_s[s, h - 1] == t, 1.0, 0.0).astype(F32)
                    term = update[pl.ds(s * piv, piv), :] * weight
                    total = term if total is None else total + term
                return total

            def swap(index, start, count):
                span = pl.ds(start, count)
                send(
                    swap_send.at[span],
                    swap_recv.at[span],
                    own["swap_send_sem"].at[h - 1, index],
                    own["swap_recv_sem"].at[h - 1, index],
                    partner,
                )

            swap_send[pl.ds(0, piv), :] = mixed(slots).astype(BF16)
            swap(0, 0, piv)
            if not at_root:
                for t in (1, 2):
                    swap_send[pl.ds(t * piv, piv), :] = mixed(slots + t).astype(BF16)
                swap(1, piv, 2 * piv)
                for t in (1, 2):
                    kept[pl.ds((t - 1) * piv, piv), :] = mixed(t)
            own["part_own"][pl.ds(0, piv), :] = mixed(0)
            yield SWAP
            with jax.named_scope(f"swap{h}c{c}"):
                take(swap_recv.at[pl.ds(0, piv)], own["swap_recv_sem"].at[h - 1, 0])
            front = own["part_own"][pl.ds(0, piv), :] + swap_recv[pl.ds(0, piv), :].astype(F32)
            own["x_sep"][g][own_row(h), :] = (rhs_v[h - 1, :, cols].astype(F32) + front).astype(BF16)
            yield from gather(c, g, h, f"A{h}")
            with jax.named_scope(f"productA{h}c{c}"):
                loaded(("a", h))
                products(c, g, a_v[h - 1], piv, h)
            yield PARTS_A[h - 1]
            solved = summed(c, g, piv, h, f"A{h}").astype(BF16)
            last = g + 1
            solved_row = rows(blk * piv, piv)
            own["x_sep"][last][solved_row, :] = solved
            write(
                own["x_sep"][last].at[solved_row], sep_out.at[h - 1, :, cols], own["out_sem"].at[h]
            )
            if not at_root:
                yield from gather(c, last, h, f"L{h}")
                with jax.named_scope(f"productL{h}c{c}"):
                    loaded(("l", h))
                    products(c, last, l_v[h - 1], 2 * piv, h)
                yield PARTS_L[h - 1]
                product = summed(c, last, 2 * piv, h, f"L{h}")
                take(swap_recv.at[pl.ds(piv, 2 * piv)], own["swap_recv_sem"].at[h - 1, 1])
                update[...] = (
                    kept[...] + swap_recv[pl.ds(piv, 2 * piv), :].astype(F32)
                ) - product

    bulk = bulk_plan(levels, piv)
    running = {c: chain(c) for c in range(CHAINS)}
    ready = {c: c * LEAD for c in range(CHAINS)}
    now = 0.0
    while running:
        c = min(running, key=lambda k: ready[k])
        now = max(now, ready[c])
        try:
            ready[c] = now + next(running[c])
        except StopIteration:
            del running[c]
        while bulk and bulk[0][0] <= now:
            send_block(*bulk.pop(0)[1])

    for c in range(CHAINS):
        own = chains[c]
        for phase in (0, 1):
            total = chunks * (2 * nz - 1) * CHUNK
            take(own["x_leaf"][phase].at[pl.ds(0, total)], own["leaf_send_sem"].at[phase])
        for h in range(1, levels + 1):
            for kind in (0, 1):
                if kind == 1 and h == levels:
                    continue
                g = 2 * (h - 1) + kind
                count = piv * (1 + kind)
                blocks = 2 * nz * (NX if wide_level(h, levels) else 1) - 1
                others = len(masks_of(h, levels)) - 1
                take(own["x_sep"][g].at[pl.ds(0, blocks * piv)], own["gather_send_sem"].at[g])
                take(
                    own["part_send"][g].at[pl.ds(count, others * count)],
                    own["part_send_sem"].at[g],
                )
                span = pl.ds(kind * piv, count)
                take(own["swap_send"][h - 1].at[span], own["swap_send_sem"].at[h - 1, kind])
    for h in range(1, levels + 1):
        for kind in ("a", "l"):
            if kind == "l" and h == levels:
                continue
            source, target, count, index = matrix_of(kind, h)
            others = len(masks_of(h, levels)) - 1
            take(target.at[pl.ds(count, count * others)], bulk_send_sem.at[index])
    for copy in out_copies:
        copy.wait()


def bulk_plan(levels, piv):
    def pieces(kind, h, masks, size):
        count = piv if kind == "a" else 2 * piv
        size = min(size, count)
        known = masks_of(h, levels)
        return [
            (kind, h, m, f, size) for m in masks if m in known for f in range(0, count, size)
        ]

    def at(when, items):
        return [(when, item) for item in items]

    plan = []
    for h in range(1, min(levels, 3)):
        for kind in ("a", "l"):
            plan += at(0.0, pieces(kind, h, (1, 3, 2), 2 * piv))
    plan += at(0.0, pieces("a", levels, [NX * m for m in (1, 3, 2)], 2 * piv))
    if levels > 3:
        plan += at(0.0, pieces("a", 3, (4,), 2 * piv))
        plan += at(BULK_A3, pieces("a", 3, (1, 3, 2, 5, 7, 6), 2 * piv))
        plan += at(BULK_A3, pieces("l", 3, (4,), 2 * piv))
        plan += at(1e9, pieces("l", 3, (1, 3, 2, 5, 7, 6), piv // 2))
    return plan


def put_out(leaf_in, sep_in, leaf_out, sep_out, sem):
    copies = [
        pltpu.make_async_copy(leaf_in, leaf_out, sem.at[0]),
        pltpu.make_async_copy(sep_in, sep_out, sem.at[1]),
    ]
    for copy in copies:
        copy.start()
    for copy in copies:
        copy.wait()


def on_device(sizes, leaf_rhs, leaf_inverse, leaf_lower, sep_rhs, sep_inverse, sep_lower, slot_map):
    n_leaf, n_blk, levels = sizes
    leaf_rows, columns = leaf_rhs.shape
    chunks = leaf_rows // CHUNK
    nz = n_blk // CORES
    piv = sep_rhs.shape[1]
    base = piv * n_blk
    gathers = 2 * levels - 1
    slots = slot_map[:, 0, :].T

    def level_of(g):
        return g // 2 + 1

    def count_of(g):
        return piv * (1 + g % 2)

    vmem, dma = pltpu.VMEM, pltpu.SemaphoreType.DMA
    width = columns // CHAINS

    def parts():
        return [
            vmem((count_of(g) * len(masks_of(level_of(g), levels)), width), BF16)
            for g in range(gathers)
        ]

    def swaps():
        return [vmem((3 * piv, width), BF16) for _ in range(levels)]

    def scratch_of_chain():
        return {
            "x_leaf": [vmem((leaf_rows * n_blk, width), BF16) for _ in range(2)],
            "acc": vmem((leaf_rows, width), F32),
            "x_sep": [
                vmem((base * (NX if g < gathers and wide_level(level_of(g), levels) else 1), width), BF16)
                for g in range(gathers + 1)
            ],
            "part_own": vmem((2 * piv, width), F32),
            "part_send": parts(),
            "part_recv": parts(),
            "update": vmem((2 * piv, width), F32),
            "swap_send": swaps(),
            "swap_recv": swaps(),
            "kept": vmem((2 * piv, width), F32),
            "out_sem": dma((1 + levels,)),
            "ring_sem": dma((2, 2, nz // 2, chunks)),
            "leaf_sib_sem": dma((2, nz)),
            "leaf_send_sem": dma((2,)),
            "z_sem": dma((gathers, nz)),
            "x_sem": dma((NX, 2)),
            "sib_sem": dma((gathers,)),
            "gather_send_sem": dma((gathers,)),
            "part_recv_sem": dma((gathers,)),
            "part_send_sem": dma((gathers,)),
            "swap_recv_sem": dma((levels, 2)),
            "swap_send_sem": dma((levels, 2)),
        }

    any_space = pl.BlockSpec(memory_space=pl.ANY)
    leaf_out, sep_out = pl.pallas_call(
        functools.partial(kernel, sizes),
        out_shape=(
            jax.ShapeDtypeStruct((leaf_rows, columns), BF16),
            jax.ShapeDtypeStruct((levels, piv, columns), BF16),
        ),
        in_specs=[any_space] * 7,
        out_specs=(pl.BlockSpec(memory_space=pltpu.VMEM),) * 2,
        scratch_shapes=[
            vmem(leaf_inverse.shape, BF16),
            vmem(leaf_lower.shape, BF16),
            vmem(sep_rhs.shape, BF16),
            pltpu.SMEM(slots.shape, jnp.int32),
            [
                vmem(
                    (piv * len(masks_of(h, levels)), base * 2**h // len(masks_of(h, levels))), BF16
                )
                for h in range(1, levels + 1)
            ],
            [vmem((2 * piv * 2**h, base), BF16) for h in range(1, levels)],
            [scratch_of_chain() for _ in range(CHAINS)],
            dma((CHAINS + 4 + 2 * levels,)),
            dma((gathers,)),
            dma((gathers,)),
        ],
        compiler_params=pltpu.CompilerParams(
            collective_id=0, has_side_effects=True, vmem_limit_bytes=60 * 2**20
        ),
    )(leaf_rhs, leaf_inverse, leaf_lower, sep_rhs, sep_inverse, sep_lower, slots)
    return pl.pallas_call(
        put_out,
        out_shape=(
            jax.ShapeDtypeStruct((leaf_rows, columns), BF16),
            jax.ShapeDtypeStruct((levels, piv, columns), BF16),
        ),
        in_specs=[pl.BlockSpec(memory_space=pltpu.VMEM)] * 2,
        out_specs=(any_space, any_space),
        scratch_shapes=[dma((2,))],
    )(leaf_out, sep_out)


def solution(mesh):
    n_leaf, n_blk = mesh.shape["leaf"], mesh.shape["blk"]
    sizes = (n_leaf, n_blk, n_leaf.bit_length() - 1)
    return jax.shard_map(
        functools.partial(on_device, sizes),
        mesh=mesh,
        in_specs=(
            P(("leaf", "blk"), None),
            P(("leaf", "blk"), None),
            P(("leaf", "blk"), None),
            P(None, ("leaf", "blk"), None),
            P(("leaf", "blk"), None),
            P(("leaf", "blk"), None),
            P(None, ("leaf", "blk"), None),
        ),
        out_specs=(P(("leaf", "blk"), None), P(None, ("leaf", "blk"), None)),
        check_vma=False,
    )
```

```python
import functools

import jax
import jax.numpy as jnp
from jax import lax
from jax.experimental import pallas as pl
from jax.experimental.pallas import tpu as pltpu
from jax.sharding import PartitionSpec as P

MESH = pl.DeviceIdType.MESH
F32 = jnp.float32
BF16 = jnp.bfloat16
CORES = 2
NX = 4
SEND_GATHERS = 3
CHUNK = 160
CHAINS = 2
LEAD = 0.0
LEAF_HOP = 2.9
SIBLING = 0.0
LEAF_SIBLING = 1.0
GATHER = 5.5
SWAP = 2.6
PARTS_A = (2.6, 3.3, 4.5, 6.0)
PARTS_L = (3.0, 4.0, 6.0)
BULK_A3 = 6.0
GATHER_X = (0.5, 0.0)
BULK_ROOM = (8, 4, 7, 7, 6, 4, 0)


def flipped(index, mask):
    result = index
    bit = 1
    while bit <= mask:
        if mask & bit:
            result = result + (bit - 2 * bit * lax.rem(lax.div(index, bit), 2))
        bit *= 2
    return result


def wide_level(h, levels):
    return h == levels


def masks_of(h, levels):
    return [m for m in range(2**h) if not wide_level(h, levels) or m % NX == 0]


def send_group(g):
    return 2 + g // SEND_GATHERS


def take(ref, sem):
    pltpu.make_async_copy(ref, ref, sem).wait()


def rows(start, count):
    return pl.ds(pl.multiple_of(start, count), count)


def kernel(
    sizes,
    leaf_rhs,
    leaf_inverse,
    leaf_lower,
    sep_rhs,
    sep_inverse,
    sep_lower,
    slot_map,
    leaf_out,
    sep_out,
    inv_v,
    low_v,
    rhs_v,
    map_s,
    a_v,
    l_v,
    chains,
    load_sem,
    bulk_recv_sem,
    bulk_send_sem,
):
    n_leaf, n_blk, levels = sizes
    nz = n_blk // CORES
    half = nz // 2
    leaf = lax.axis_index("leaf")
    blk = lax.axis_index("blk")
    z = lax.div(blk, CORES)
    core = lax.rem(blk, CORES)
    sibling = (leaf, flipped(blk, 1))
    leaf_rows, columns = leaf_rhs.shape
    width = columns // CHAINS
    chunks = leaf_rows // CHUNK
    chip_rows = leaf_rows * CORES
    piv = sep_rhs.shape[1]
    base = piv * n_blk
    own_leaf = rows(blk * leaf_rows, leaf_rows)

    def own_row(h):
        if wide_level(h, levels):
            return rows(lax.rem(leaf, NX) * base + blk * piv, piv)
        return rows(blk * piv, piv)

    def columns_for(h, member):
        index = lax.rem(member, 2**h)
        span = base
        if wide_level(h, levels):
            index, span = lax.div(index, NX), base * NX
        return pl.ds(pl.multiple_of(base * (2**h - 2) + span * index, base), span)

    def at_z(distance):
        return lax.rem(z + (distance + nz), nz)

    def columns_of(c):
        return pl.ds(c * width, width)

    loads = {}

    def load(key, source, target):
        loads[key] = pltpu.make_async_copy(source, target, load_sem.at[len(loads)])
        loads[key].start()

    waited = set()

    def loaded(key):
        if key not in waited:
            waited.add(key)
            loads[key].wait()
            if key[0] in ("a", "l"):
                while any(item[:2] == key for _, item in bulk):
                    send_block(*bulk.pop(0)[1])
                with jax.named_scope(f"blocks{key[0]}{key[1]}"):
                    wait_blocks(*key)

    for c in range(CHAINS):
        load(("rhs", c), leaf_rhs.at[:, columns_of(c)], chains[c]["x_leaf"][0].at[own_leaf])
    load(("inverse",), leaf_inverse, inv_v)
    load(("lower",), leaf_lower, low_v)
    load(("sep_rhs",), sep_rhs, rhs_v)
    load(("map",), slot_map, map_s)
    for h in range(1, levels + 1):
        own = columns_for(h, leaf)
        load(("a", h), sep_inverse.at[:, own], a_v[h - 1].at[pl.ds(0, piv)])
        if h < levels:
            load(("l", h), sep_lower.at[:, own], l_v[h - 1].at[pl.ds(0, 2 * piv)])

    barrier = pltpu.get_barrier_semaphore()
    peers = [sibling]
    peers += [(leaf, at_z(d) * CORES + core) for d in range(1, nz)]
    peers += [(flipped(leaf, m), blk) for m in range(1, n_leaf)]
    for peer in peers:
        pl.semaphore_signal(barrier, inc=1, device_id=peer, device_id_type=MESH)
    for c in range(CHAINS):
        loaded(("rhs", c))
    with jax.named_scope("entry"):
        pl.semaphore_wait(barrier, len(peers))

    def send(src, dst, send_sem, recv_sem, device):
        pltpu.make_async_remote_copy(
            src_ref=src,
            dst_ref=dst,
            send_sem=send_sem,
            recv_sem=recv_sem,
            device_id=device,
            device_id_type=MESH,
        ).start()

    def matrix_of(kind, h):
        if kind == "a":
            return sep_inverse, a_v[h - 1], piv, 2 * (h - 1)
        return sep_lower, l_v[h - 1], 2 * piv, 2 * (h - 1) + 1

    def send_block(kind, h, m, first, size):
        source, target, count, index = matrix_of(kind, h)
        peer = flipped(leaf, m)
        size = min(size, count)
        slot = masks_of(h, levels).index(m)
        send(
            source.at[pl.ds(first, size), columns_for(h, peer)],
            target.at[pl.ds(slot * count + first, size)],
            bulk_send_sem.at[index],
            bulk_recv_sem.at[index],
            (peer, blk),
        )

    def wait_blocks(kind, h):
        source, target, count, index = matrix_of(kind, h)
        others = len(masks_of(h, levels)) - 1
        take(target.at[pl.ds(count, count * others)], bulk_recv_sem.at[index])

    def blocks_beside(g):
        room = BULK_ROOM[g]
        while bulk and room > 0:
            item = bulk.pop(0)[1]
            send_block(*item)
            room -= (0, 1, 2, 1)[item[2] % 4]

    def each(first, last, body):
        def run(chunk, carry):
            body(chunk)
            return carry

        lax.fori_loop(first, last, run, 0)

    def leaf_gather(c, phase, multiply):
        own = chains[c]
        x = own["x_leaf"][phase]
        send_sem = own["send_sem"].at[phase]

        def chunk_at(slot, chunk):
            return x.at[rows((slot * CORES + core) * leaf_rows + chunk * CHUNK, CHUNK)]

        def hop(way, step, chunk):
            sign = 1 if way == 0 else -1
            block = chunk_at(at_z(-sign * (step - 1)), chunk)
            send(
                block,
                block,
                send_sem,
                own["ring_sem"].at[phase, way, step - 1, chunk],
                (leaf, at_z(sign) * CORES + core),
            )

        def to_sibling(slot, sem_index, chunk):
            block = chunk_at(slot, chunk)
            send(block, block, send_sem, own["leaf_sib_sem"].at[phase, sem_index], sibling)

        def arrived(way, step, chunk):
            sign = 1 if way == 0 else -1
            slot = at_z(-sign * step)
            take(chunk_at(slot, chunk), own["ring_sem"].at[phase, way, step - 1, chunk])
            to_sibling(slot, step, chunk)

        split = (chunks + c) // 2 if CHAINS > 1 else (chunks + 1) // 2

        def begin(chunk):
            hop(0, 1, chunk)
            hop(1, 1, chunk)
            to_sibling(z, 0, chunk)

        def finish(step):
            ways = (step,) if step in (0, half) else (-step, step)
            take(x.at[pl.ds(0, len(ways) * leaf_rows)], own["leaf_sib_sem"].at[phase, step])
            for distance in ways:
                multiply(at_z(distance), distance == 0)

        each(0, chunks, begin)
        yield LEAF_HOP
        for step in range(1, half):
            with jax.named_scope(f"leaf{phase}c{c}s{step}"):
                if step + 1 < half:

                    def both(chunk, step=step):
                        for way in (0, 1):
                            arrived(way, step, chunk)
                            hop(way, step + 1, chunk)

                    each(0, chunks, both)
                else:

                    def low(chunk, step=step):
                        arrived(0, step, chunk)
                        hop(0, step + 1, chunk)
                        arrived(1, step, chunk)

                    def high(chunk, step=step):
                        arrived(1, step, chunk)
                        hop(1, step + 1, chunk)
                        arrived(0, step, chunk)

                    each(0, split, low)
                    each(split, chunks, high)
            with jax.named_scope(f"leafm{phase}c{c}s{step}"):
                finish(step - 1)
            yield LEAF_HOP
        finish(half - 1)
        with jax.named_scope(f"leaf{phase}c{c}s{half}"):
            each(0, split, lambda chunk: arrived(0, half, chunk))
            each(split, chunks, lambda chunk: arrived(1, half, chunk))
        yield LEAF_SIBLING
        with jax.named_scope(f"leafm{phase}c{c}s{half}"):
            finish(half)

    def gather(c, g, h, name):
        own = chains[c]
        wide = wide_level(h, levels)
        x = own["x_sep"][g]
        part = lax.rem(leaf, NX) * base if wide else 0

        def block(slot, start=part):
            return x.at[rows(start + (slot * CORES + core) * piv, piv)]

        def push(ref, sem, device):
            send(ref, ref, own["send_sem"].at[send_group(g)], sem, device)

        def to_sibling(ref):
            push(ref, own["sib_sem"].at[g], sibling)

        near = sorted(range(1, nz), key=lambda d: min(d, nz - d))
        halves = (near[: nz // 2], near[nz // 2 :])
        x_halves = ([0] + halves[0], halves[1])

        def along_x(d):
            if wide:
                for m in (1, 3, 2):
                    if m < NX:
                        sem = own["x_sem"].at[m - 1, 1 if d in halves[1] else 0]
                        push(block(at_z(-d)), sem, (flipped(leaf, m), blk))

        for d in reversed(near):
            sem = own["z_sem"].at[g, 1 if d in halves[1] else 0]
            push(block(z), sem, (leaf, at_z(d) * CORES + core))
        to_sibling(block(z))
        along_x(0)
        if c == CHAINS - 1:
            blocks_beside(g)

        yield GATHER
        with jax.named_scope(f"far{name}c{c}"):
            for index in (0, 1):
                take(x.at[pl.ds(0, len(halves[index]) * piv)], own["z_sem"].at[g, index])
                for d in halves[index]:
                    along_x(d)
                    to_sibling(block(at_z(-d)))
        if wide:
            for half_index in (0, 1):
                yield GATHER_X[half_index]
                with jax.named_scope(f"x{half_index}{name}c{c}"):
                    for m in (1, 3, 2):
                        if m < NX:
                            take(
                                x.at[pl.ds(0, len(x_halves[half_index]) * piv)],
                                own["x_sem"].at[m - 1, half_index],
                            )
                            start = lax.rem(flipped(leaf, m), NX) * base
                            for d in x_halves[half_index]:
                                to_sibling(block(at_z(-d), start))
        yield SIBLING
        with jax.named_scope(f"sib{name}c{c}"):
            take(x.at[pl.ds(0, nz * piv * (NX if wide else 1))], own["sib_sem"].at[g])

    def products(c, g, matrix, count, h):
        own = chains[c]
        masks = masks_of(h, levels)
        members = len(masks)
        per = max(1, min(members, 256 // count))
        out, mine = own["part_send"][g], own["part_own"].at[pl.ds(0, count)]
        x = own["x_sep"][g]
        for first in reversed(range(0, members, per)):
            span = pl.ds(first * count, per * count)
            value = jnp.dot(matrix[span, :], x[...], preferred_element_type=F32)
            out[span, :] = value.astype(BF16)
            if first == 0:
                mine[...] = value[:count]
            for m in range(max(first, 1), first + per):
                slot = pl.ds(m * count, count)
                send(
                    out.at[slot],
                    own["part_recv"][g].at[slot],
                    own["send_sem"].at[send_group(g)],
                    own["part_recv_sem"].at[g],
                    (flipped(leaf, masks[m]), blk),
                )

    def summed(c, g, count, h, name):
        own = chains[c]
        members = len(masks_of(h, levels))
        with jax.named_scope(f"parts{name}c{c}"):
            take(
                own["part_recv"][g].at[pl.ds(count, (members - 1) * count)],
                own["part_recv_sem"].at[g],
            )
        total = own["part_own"][pl.ds(0, count), :]
        for m in range(1, members):
            total += own["part_recv"][g][pl.ds(m * count, count), :].astype(F32)
        return total

    def chain(c):
        own = chains[c]
        cols = columns_of(c)
        acc, update, kept = own["acc"], own["update"], own["kept"]

        def multiply_inverse(slot, first):
            loaded(("inverse",))
            span = rows(slot * chip_rows, chip_rows)
            value = jnp.dot(inv_v[:, span], own["x_leaf"][0][span, :], preferred_element_type=F32)
            acc[...] = value if first else acc[...] + value

        def multiply_lower(slot, first):
            loaded(("lower",))
            span = rows(slot * chip_rows, chip_rows)
            value = jnp.dot(low_v[:, span], own["x_leaf"][1][span, :], preferred_element_type=F32)
            update[...] = -value if first else update[...] - value

        yield from leaf_gather(c, 0, multiply_inverse)
        own["x_leaf"][1][own_leaf, :] = acc[...].astype(BF16)
        yield from leaf_gather(c, 1, multiply_lower)
        leaf_out[:, cols] = own["x_leaf"][1][own_leaf, :]

        for h in range(1, levels + 1):
            at_root = h == levels
            slots = 1 if at_root else 3
            g = 2 * (h - 1)
            partner = (flipped(leaf, 2 ** (h - 1)), blk)
            swap_send, swap_recv = own["swap_send"][h - 1], own["swap_recv"][h - 1]
            loaded(("map",))
            loaded(("sep_rhs",))

            def mixed(t):
                total = None
                for s in (0, 1):
                    weight = jnp.where(map_s[s, h - 1] == t, 1.0, 0.0).astype(F32)
                    term = update[pl.ds(s * piv, piv), :] * weight
                    total = term if total is None else total + term
                return total

            def swap(index, start, count):
                span = pl.ds(start, count)
                send(
                    swap_send.at[span],
                    swap_recv.at[span],
                    own["send_sem"].at[send_group(g)],
                    own["swap_recv_sem"].at[h - 1, index],
                    partner,
                )

            swap_send[pl.ds(0, piv), :] = mixed(slots).astype(BF16)
            swap(0, 0, piv)
            if not at_root:
                for t in (1, 2):
                    swap_send[pl.ds(t * piv, piv), :] = mixed(slots + t).astype(BF16)
                swap(1, piv, 2 * piv)
                for t in (1, 2):
                    kept[pl.ds((t - 1) * piv, piv), :] = mixed(t)
            own["part_own"][pl.ds(0, piv), :] = mixed(0)
            yield SWAP
            with jax.named_scope(f"swap{h}c{c}"):
                take(swap_recv.at[pl.ds(0, piv)], own["swap_recv_sem"].at[h - 1, 0])
            front = own["part_own"][pl.ds(0, piv), :] + swap_recv[pl.ds(0, piv), :].astype(F32)
            own["x_sep"][g][own_row(h), :] = (rhs_v[h - 1, :, cols].astype(F32) + front).astype(BF16)
            yield from gather(c, g, h, f"A{h}")
            with jax.named_scope(f"productA{h}c{c}"):
                loaded(("a", h))
                products(c, g, a_v[h - 1], piv, h)
            yield PARTS_A[h - 1]
            solved = summed(c, g, piv, h, f"A{h}").astype(BF16)
            last = g + 1
            sep_out[h - 1, :, cols] = solved
            if not at_root:
                own["x_sep"][last][own_row(h), :] = solved
                yield from gather(c, last, h, f"L{h}")
                with jax.named_scope(f"productL{h}c{c}"):
                    loaded(("l", h))
                    products(c, last, l_v[h - 1], 2 * piv, h)
                yield PARTS_L[h - 1]
                product = summed(c, last, 2 * piv, h, f"L{h}")
                take(swap_recv.at[pl.ds(piv, 2 * piv)], own["swap_recv_sem"].at[h - 1, 1])
                update[...] = (
                    kept[...] + swap_recv[pl.ds(piv, 2 * piv), :].astype(F32)
                ) - product

    bulk = bulk_plan(levels, piv)
    running = {c: chain(c) for c in range(CHAINS)}
    ready = {c: c * LEAD for c in range(CHAINS)}
    now = 0.0
    while running:
        c = min(running, key=lambda k: ready[k])
        now = max(now, ready[c])
        try:
            ready[c] = now + next(running[c])
        except StopIteration:
            del running[c]
        while bulk and bulk[0][0] <= now:
            send_block(*bulk.pop(0)[1])

    for c in range(CHAINS):
        own = chains[c]
        total = {phase: chunks * (2 * nz - 1) * CHUNK for phase in (0, 1)}
        for h in range(1, levels + 1):
            for kind in (0, 1):
                if kind == 1 and h == levels:
                    continue
                g = 2 * (h - 1) + kind
                count = piv * (1 + kind)
                group = send_group(g)
                blocks = 2 * nz * (NX if wide_level(h, levels) else 1) - 1
                others = len(masks_of(h, levels)) - 1
                total[group] = total.get(group, 0) + blocks * piv + others * count
                group = send_group(2 * (h - 1))
                total[group] = total.get(group, 0) + count
        for group, amount in total.items():
            take(own["x_leaf"][0].at[pl.ds(0, amount)], own["send_sem"].at[group])
    for h in range(1, levels + 1):
        for kind in ("a", "l"):
            if kind == "l" and h == levels:
                continue
            source, target, count, index = matrix_of(kind, h)
            others = len(masks_of(h, levels)) - 1
            take(target.at[pl.ds(count, count * others)], bulk_send_sem.at[index])


def bulk_plan(levels, piv):
    def pieces(kind, h, masks, size):
        count = piv if kind == "a" else 2 * piv
        size = min(size, count)
        known = masks_of(h, levels)
        return [
            (kind, h, m, f, size) for m in masks if m in known for f in range(0, count, size)
        ]

    def at(when, items):
        return [(when, item) for item in items]

    plan = []
    for h in range(1, min(levels, 3)):
        for kind in ("a", "l"):
            plan += at(0.0, pieces(kind, h, (1, 3, 2), 2 * piv))
    plan += at(0.0, pieces("a", levels, [NX * m for m in (1, 3, 2)], 2 * piv))
    if levels > 3:
        plan += at(0.0, pieces("a", 3, (4,), 2 * piv))
        plan += at(BULK_A3, pieces("a", 3, (2, 6, 1, 5), 2 * piv))
        plan += at(BULK_A3, pieces("l", 3, (4,), 2 * piv))
        plan += at(1e9, pieces("l", 3, (3, 7), piv // 2))
        plan += at(1e9, pieces("a", 3, (3, 7), piv // 2))
        mixed = zip(*(pieces("l", 3, (m,), piv // 2) for m in (2, 1, 6, 5)))
        plan += at(1e9, [item for group in mixed for item in group])
    return plan


def put_out(leaf_in, sep_in, leaf_out, sep_out, sem):
    copies = [
        pltpu.make_async_copy(leaf_in, leaf_out, sem.at[0]),
        pltpu.make_async_copy(sep_in, sep_out, sem.at[1]),
    ]
    for copy in copies:
        copy.start()
    for copy in copies:
        copy.wait()


def on_device(sizes, leaf_rhs, leaf_inverse, leaf_lower, sep_rhs, sep_inverse, sep_lower, slot_map):
    n_leaf, n_blk, levels = sizes
    leaf_rows, columns = leaf_rhs.shape
    chunks = leaf_rows // CHUNK
    nz = n_blk // CORES
    piv = sep_rhs.shape[1]
    base = piv * n_blk
    gathers = 2 * levels - 1
    slots = slot_map[:, 0, :].T

    def level_of(g):
        return g // 2 + 1

    def count_of(g):
        return piv * (1 + g % 2)

    vmem, dma = pltpu.VMEM, pltpu.SemaphoreType.DMA
    width = columns // CHAINS

    def parts():
        return [
            vmem((count_of(g) * len(masks_of(level_of(g), levels)), width), BF16)
            for g in range(gathers)
        ]

    def swaps():
        return [vmem((3 * piv, width), BF16) for _ in range(levels)]

    def scratch_of_chain():
        return {
            "x_leaf": [vmem((leaf_rows * n_blk, width), BF16) for _ in range(2)],
            "acc": vmem((leaf_rows, width), F32),
            "x_sep": [
                vmem((base * (NX if g < gathers and wide_level(level_of(g), levels) else 1), width), BF16)
                for g in range(gathers + 1)
            ],
            "part_own": vmem((2 * piv, width), F32),
            "part_send": parts(),
            "part_recv": parts(),
            "update": vmem((2 * piv, width), F32),
            "swap_send": swaps(),
            "swap_recv": swaps(),
            "kept": vmem((2 * piv, width), F32),
            "ring_sem": dma((2, 2, nz // 2, chunks)),
            "leaf_sib_sem": dma((2, nz // 2 + 1)),
            "send_sem": dma((3 + (gathers - 1) // SEND_GATHERS,)),
            "z_sem": dma((gathers, 2)),
            "x_sem": dma((NX - 1, 2)),
            "sib_sem": dma((gathers,)),
            "part_recv_sem": dma((gathers,)),
            "swap_recv_sem": dma((levels, 2)),
        }

    any_space = pl.BlockSpec(memory_space=pl.ANY)
    leaf_out, sep_out = pl.pallas_call(
        functools.partial(kernel, sizes),
        out_shape=(
            jax.ShapeDtypeStruct((leaf_rows, columns), BF16),
            jax.ShapeDtypeStruct((levels, piv, columns), BF16),
        ),
        in_specs=[any_space] * 7,
        out_specs=(pl.BlockSpec(memory_space=pltpu.VMEM),) * 2,
        scratch_shapes=[
            vmem(leaf_inverse.shape, BF16),
            vmem(leaf_lower.shape, BF16),
            vmem(sep_rhs.shape, BF16),
            pltpu.SMEM(slots.shape, jnp.int32),
            [
                vmem(
                    (piv * len(masks_of(h, levels)), base * 2**h // len(masks_of(h, levels))), BF16
                )
                for h in range(1, levels + 1)
            ],
            [vmem((2 * piv * 2**h, base), BF16) for h in range(1, levels)],
            [scratch_of_chain() for _ in range(CHAINS)],
            dma((CHAINS + 4 + 2 * levels,)),
            dma((gathers,)),
            dma((gathers,)),
        ],
        compiler_params=pltpu.CompilerParams(
            collective_id=0, has_side_effects=True, vmem_limit_bytes=60 * 2**20
        ),
    )(leaf_rhs, leaf_inverse, leaf_lower, sep_rhs, sep_inverse, sep_lower, slots)
    return pl.pallas_call(
        put_out,
        out_shape=(
            jax.ShapeDtypeStruct((leaf_rows, columns), BF16),
            jax.ShapeDtypeStruct((levels, piv, columns), BF16),
        ),
        in_specs=[pl.BlockSpec(memory_space=pltpu.VMEM)] * 2,
        out_specs=(any_space, any_space),
        scratch_shapes=[dma((2,))],
    )(leaf_out, sep_out)


def solution(mesh):
    n_leaf, n_blk = mesh.shape["leaf"], mesh.shape["blk"]
    sizes = (n_leaf, n_blk, n_leaf.bit_length() - 1)
    return jax.shard_map(
        functools.partial(on_device, sizes),
        mesh=mesh,
        in_specs=(
            P(("leaf", "blk"), None),
            P(("leaf", "blk"), None),
            P(("leaf", "blk"), None),
            P(None, ("leaf", "blk"), None),
            P(("leaf", "blk"), None),
            P(("leaf", "blk"), None),
            P(None, ("leaf", "blk"), None),
        ),
        out_specs=(P(("leaf", "blk"), None), P(None, ("leaf", "blk"), None)),
        check_vma=False,
    )
```
